32 devices in a mesh: batch: 4 (over z), grid: 8 (over y, x, core).
Axes of the slice: x: 2, y: 2, z: 4, core: 2. Of those that a mesh axis runs over, the one named last changes fastest.
Arguments:
- fields: bfloat16 [1024, 512, 512], P(('batch', 'grid')), parts along dimension 0, may hold values from -18 to 18
- norm_gain: float32 [256], replicated, may hold values from 0.5 to 1.5
- norm_shift: float32 [256], replicated, may hold values from -3 to 3
- first_weight: bfloat16 [2, 8, 32, 32], replicated, may hold values from -0.75 to 0.75
- second_weight: bfloat16 [2, 8, 32, 32], replicated, may hold values from -0.75 to 0.75
- first_bias: float32 [2, 256], replicated, may hold values from -2 to 2
Outputs:
- mixed_fields: bfloat16 [1024, 512, 512], P(('batch', 'grid')), parts along dimension 0
The draws below stay inside these ranges and needn't reach their ends.
There are 4 independent parts, one for each index of `batch`. The reference program is written for one: setup_inputs(seed, part) draws one part's arguments, and reference() takes and returns one part's arrays. A program takes and returns all parts, laid end to end along the dimension named above; an argument that names none is the same for every part. Nothing has to cross between parts.
All inputs are finite; a program needn't handle non-finite values.
Results may differ from the reference program's by a relative error of at most 0.0055.
Values may be sent and summed in bfloat16 or wider, within the bound.
No kernel may reach another device: no remote copies, remote signals or barrier semaphores. Data moves between devices by JAX's collectives and lax.ppermute only.
A program may use at most 192 MiB of HBM per device.

```python
import math
import jax
import jax.numpy as jnp
from jax import lax

C = 256
BS = 32
H = 512
W = 512
NB = 8


def draw_fields(key, part):
    first_key = jax.random.fold_in(key, 11)
    ramp = jnp.arange(C, dtype=jnp.float32) / (C - 1)
    base = jnp.clip(jax.random.normal(first_key, (C, H, W), jnp.float32), -4.0, 4.0)
    scale = jnp.power(3.0, ramp)
    return (base * scale[:, None, None]).astype(jnp.bfloat16)


def normal_values(key, extent, scale, bound, kind=jnp.bfloat16):
    entries = scale * jax.random.normal(key, extent, jnp.float32)
    return jnp.clip(entries, min=-bound, max=bound).astype(kind)


def setup_inputs(seed: int = 0, part: int = 0) -> dict:
    splits = jax.random.split(jax.random.key(seed), 7)
    part_splits = jax.random.split(jax.random.fold_in(splits[6], part), 7)
    return {
        "fields": draw_fields(jax.random.fold_in(jax.random.fold_in(splits[6], part), 71), part),
        "norm_gain": jnp.clip(1.0 + 0.1 * jax.random.normal(splits[1], (C,), jnp.float32), 0.5, 1.5),
        "norm_shift": normal_values(splits[2], (C,), 0.5, 3.0, jnp.float32),
        "first_weight": normal_values(splits[3], (2, NB, BS, BS), (2 * BS) ** -0.5, 0.75),
        "second_weight": normal_values(splits[4], (2, NB, BS, BS), (2 * BS) ** -0.5, 0.75),
        "first_bias": normal_values(splits[5], (2, C), 0.3, 2.0, jnp.float32),
    }


def tables(rows, cols):
    half = cols // 2
    col_index = jnp.arange(cols, dtype=jnp.int32)
    mode_index = jnp.arange(half, dtype=jnp.int32)
    angle_w = (col_index[:, None] * mode_index[None, :] % cols).astype(jnp.float32) * (2.0 * math.pi / cols)
    scale_w = 1.0 / math.sqrt(cols)
    fwd_w = jnp.concatenate([jnp.cos(angle_w) * scale_w, -jnp.sin(angle_w) * scale_w], axis=1).astype(jnp.bfloat16)
    weight_k = jnp.where(mode_index == 0, 1.0, 2.0).astype(jnp.float32)
    inv_w = jnp.concatenate([(jnp.cos(angle_w) * weight_k[None, :] * scale_w).T, (-jnp.sin(angle_w) * weight_k[None, :] * scale_w).T], axis=0).astype(jnp.bfloat16)
    row_index = jnp.arange(rows, dtype=jnp.int32)
    angle_h = (row_index[:, None] * row_index[None, :] % rows).astype(jnp.float32) * (2.0 * math.pi / rows)
    scale_h = 1.0 / math.sqrt(rows)
    cos_h = (jnp.cos(angle_h) * scale_h).astype(jnp.bfloat16)
    sin_h = (jnp.sin(angle_h) * scale_h).astype(jnp.bfloat16)
    return (fwd_w, inv_w, cos_h, sin_h)

def mult(form, left, right):
    return jnp.einsum(form, left.astype(jnp.float32), right.astype(jnp.float32), precision=lax.Precision.HIGHEST)

def shrink(values):
    return jnp.maximum(values - 0.01, 0.0) + jnp.minimum(values + 0.01, 0.0)

def mix_modes(real_part, imag_part, first_weight, second_weight, first_bias):
    blocks = first_weight.shape[1]
    width = first_weight.shape[2]
    shape = real_part.shape
    real_blk = real_part.reshape(blocks, width, -1)
    imag_blk = imag_part.reshape(blocks, width, -1)
    bias_blk = first_bias.reshape(2, blocks, width, 1)
    hid_re = jax.nn.relu(mult('bio,bim->bom', first_weight[0], real_blk) - mult('bio,bim->bom', first_weight[1], imag_blk) + bias_blk[0]).astype(jnp.bfloat16)
    hid_im = jax.nn.relu(mult('bio,bim->bom', first_weight[0], imag_blk) + mult('bio,bim->bom', first_weight[1], real_blk) + bias_blk[1]).astype(jnp.bfloat16)
    out_re = mult('bio,bim->bom', second_weight[0], hid_re) - mult('bio,bim->bom', second_weight[1], hid_im)
    out_im = mult('bio,bim->bom', second_weight[0], hid_im) + mult('bio,bim->bom', second_weight[1], hid_re)
    return (shrink(out_re).astype(jnp.bfloat16).reshape(shape), shrink(out_im).astype(jnp.bfloat16).reshape(shape))

def reference(fields, norm_gain, norm_shift, first_weight, second_weight, first_bias):
    channels, rows, cols = fields.shape
    half = cols // 2
    fwd_w, inv_w, cos_h, sin_h = tables(rows, cols)
    values = fields.astype(jnp.float32)
    mean = lax.optimization_barrier(jnp.mean(values, axis=0))
    mean_sq = lax.optimization_barrier(jnp.mean(values * values, axis=0))
    var = mean_sq - mean * mean
    normed = ((values - mean) * lax.rsqrt(var + 1e-05) * norm_gain[:, None, None] + norm_shift[:, None, None]).astype(jnp.bfloat16)
    along_w = mult('chw,wk->chk', normed, fwd_w).astype(jnp.bfloat16).reshape(channels, rows, 2, half)
    first_p = mult('kh,chpq->ckpq', cos_h, along_w)
    first_q = mult('kh,chpq->ckpq', sin_h, along_w)
    modes_re = (first_p[:, :, 0] + first_q[:, :, 1]).astype(jnp.bfloat16)
    modes_im = (first_p[:, :, 1] - first_q[:, :, 0]).astype(jnp.bfloat16)
    shr_re, shr_im = mix_modes(modes_re, modes_im, first_weight, second_weight, first_bias)
    shrunk = jnp.stack([shr_re, shr_im], axis=2)
    back_p = mult('kh,ckpq->chpq', cos_h, shrunk)
    back_q = mult('kh,ckpq->chpq', sin_h, shrunk)
    back_re = (back_p[:, :, 0] - back_q[:, :, 1]).astype(jnp.bfloat16)
    back_im = (back_p[:, :, 1] + back_q[:, :, 0]).astype(jnp.bfloat16)
    backed = jnp.concatenate([back_re, back_im], axis=2)
    filtered = mult('chk,kw->chw', backed, inv_w)
    return (values + filtered).astype(jnp.bfloat16)
```

```python
import functools
import math

import jax
import jax.numpy as jnp
from jax import lax
from jax.experimental import pallas as pl
from jax.experimental.pallas import tpu as pltpu
from jax.sharding import PartitionSpec as P

LANES = 128
F32 = jnp.float32
BF16 = jnp.bfloat16


def tables(rows, cols):
    half = cols // 2
    col_index = jnp.arange(cols, dtype=jnp.int32)
    mode_index = jnp.arange(half, dtype=jnp.int32)
    angle_w = (col_index[:, None] * mode_index[None, :] % cols).astype(F32) * (
        2.0 * math.pi / cols
    )
    scale_w = 1.0 / math.sqrt(cols)
    fwd_w = jnp.concatenate(
        [jnp.cos(angle_w) * scale_w, -jnp.sin(angle_w) * scale_w], axis=1
    ).astype(BF16)
    weight_k = jnp.where(mode_index == 0, 1.0, 2.0).astype(F32)
    inv_w = jnp.concatenate(
        [
            (jnp.cos(angle_w) * weight_k[None, :] * scale_w).T,
            (-jnp.sin(angle_w) * weight_k[None, :] * scale_w).T,
        ],
        axis=0,
    ).astype(BF16)
    mid = rows // 2
    row_index = jnp.arange(rows, dtype=jnp.int32)
    k_index = jnp.arange(mid, dtype=jnp.int32)
    angle_h = (k_index[:, None] * row_index[None, :] % rows).astype(F32) * (2.0 * math.pi / rows)
    scale_h = 1.0 / math.sqrt(rows)
    nyquist = jnp.where(row_index % 2 == 0, scale_h, -scale_h).astype(F32)
    cos_h = jnp.cos(angle_h) * scale_h
    sin_h = jnp.where(k_index[:, None] == 0, nyquist[None, :], jnp.sin(angle_h) * scale_h)
    half_h = jnp.concatenate([cos_h, sin_h], axis=0).astype(BF16)
    return fwd_w, inv_w, half_h, half_h.T


def forward_kernel(gain, shift, x, mean, rstd, fwd_w, half_h, out):
    c = pl.program_id(0)
    mid = out.shape[2]
    half = out.shape[3] // 2
    values = x[0].astype(F32)
    normed = ((values - mean[...]) * rstd[...] * gain[c] + shift[c]).astype(BF16)
    along = jnp.dot(normed, fwd_w[...], preferred_element_type=F32).astype(BF16)
    both = jnp.dot(half_h[...], along, preferred_element_type=F32)
    c_re, c_im = both[:mid, :half], both[:mid, half:]
    s_re, s_im = both[mid:, :half], both[mid:, half:]
    first = lax.broadcasted_iota(jnp.int32, c_re.shape, 0) == 0
    out[0, 0, :, :half] = jnp.where(first, c_re, c_re + s_im).astype(BF16)
    out[0, 0, :, half:] = jnp.where(first, c_im, c_im - s_re).astype(BF16)
    out[0, 1, :, :half] = jnp.where(first, s_re, c_re - s_im).astype(BF16)
    out[0, 1, :, half:] = jnp.where(first, s_im, c_im + s_re).astype(BF16)


def shrink(values):
    return jnp.maximum(values - 0.01, 0.0) + jnp.minimum(values + 0.01, 0.0)


def mix_kernel(has_zero, x, w1, w2, bias, out, src, dst, *, rep):
    width, _, kt, cols = x.shape
    half = cols // 2
    chunks = cols // LANES
    hc = chunks // 2
    for ab in range(2):
        for l in range(chunks):
            src[ab, l] = (
                x[:, ab, :, l * LANES : (l + 1) * LANES].astype(F32).reshape(width * kt, LANES)
            )
    for ab in range(2):
        for k0 in range(0, kt, rep):
            rows = []
            for k in range(k0, k0 + rep):
                for ri in range(2):
                    rows.append(
                        jnp.concatenate(
                            [
                                src[ab, ri * hc + l, pl.ds(k, width, stride=kt), :]
                                for l in range(hc)
                            ],
                            axis=1,
                        )
                    )
            stack = jnp.concatenate(rows, axis=0).astype(BF16)
            hid = jnp.dot(w1[0], stack, preferred_element_type=F32) + bias[0]
            hid = jnp.maximum(hid, 0.0).astype(BF16)
            res = shrink(jnp.dot(w2[0], hid, preferred_element_type=F32))
            for i in range(rep):
                for ri in range(2):
                    r0 = (i * 2 + ri) * width
                    for l in range(hc):
                        dst[ab, ri * hc + l, pl.ds(k0 + i, width, stride=kt), :] = res[
                            r0 : r0 + width, l * LANES : (l + 1) * LANES
                        ]
    row = lax.broadcasted_iota(jnp.int32, (width, kt, LANES), 1)
    first = (row == 0) & ((pl.program_id(1) == 0) & (has_zero[0] == 1))
    for l in range(hc):
        shape = (width, kt, LANES)
        a_re, b_re = dst[0, l].reshape(shape), dst[1, l].reshape(shape)
        a_im, b_im = dst[0, hc + l].reshape(shape), dst[1, hc + l].reshape(shape)
        lo = slice(l * LANES, (l + 1) * LANES)
        hi = slice(half + l * LANES, half + (l + 1) * LANES)
        out[:, 0, :, lo] = jnp.where(first, a_re, a_re + b_re).astype(BF16)
        out[:, 0, :, hi] = jnp.where(first, a_im, a_im + b_im).astype(BF16)
        out[:, 1, :, lo] = jnp.where(first, b_re, b_im - a_im).astype(BF16)
        out[:, 1, :, hi] = jnp.where(first, b_im, a_re - b_re).astype(BF16)


def inverse_kernel(y, x, half_t, inv_w, out):
    rows, cols = y.shape[1] * y.shape[2], y.shape[3]
    back = jnp.dot(half_t[...], y[0].reshape(rows, cols), preferred_element_type=F32).astype(BF16)
    filtered = jnp.dot(back, inv_w[...], preferred_element_type=F32)
    out[0] = (x[0].astype(F32) + filtered).astype(BF16)


def real_form(weight, rep):
    re = jnp.swapaxes(weight[0], 1, 2)
    im = jnp.swapaxes(weight[1], 1, 2)
    whole = jnp.concatenate(
        [jnp.concatenate([re, -im], axis=2), jnp.concatenate([im, re], axis=2)], axis=1
    )
    n, size, _ = whole.shape
    eye = jnp.eye(rep, dtype=whole.dtype)
    return (eye[None, :, None, :, None] * whole[:, None, :, None, :]).reshape(
        n, rep * size, rep * size
    )


def per_device(fields, norm_gain, norm_shift, first_weight, second_weight, first_bias):
    local_ch, rows, cols = fields.shape
    half, mid = cols // 2, rows // 2
    groups = lax.axis_size("grid")
    channels = local_ch * groups
    width = first_weight.shape[2]
    fwd_w, inv_w, half_h, half_t = tables(rows, cols)
    position = lax.axis_index("grid")
    start = position * local_ch
    gain_own = lax.dynamic_slice_in_dim(norm_gain, start, local_ch)
    shift_own = lax.dynamic_slice_in_dim(norm_shift, start, local_ch)
    values = fields.astype(F32)
    total_sum, total_sq = lax.psum(
        (jnp.sum(values, axis=0), jnp.sum(values * values, axis=0)), "grid"
    )
    mean = total_sum / channels
    rstd = lax.rsqrt(total_sq / channels - mean * mean + 1e-05)

    whole = lambda shape: pl.BlockSpec(shape, lambda *_: (0,) * len(shape))
    one = pl.BlockSpec((1, rows, cols), lambda c: (c, 0, 0))
    one4 = pl.BlockSpec((1, 2, mid, cols), lambda c: (c, 0, 0, 0))
    smem = pl.BlockSpec(memory_space=pltpu.SMEM)
    flops = 4 * local_ch * rows * cols * cols
    modes = pl.pallas_call(
        forward_kernel,
        grid=(local_ch,),
        in_specs=[smem, smem, one, whole((rows, cols)), whole((rows, cols)),
                  whole((cols, cols)), whole((rows, rows))],
        out_specs=one4,
        out_shape=jax.ShapeDtypeStruct((local_ch, 2, mid, cols), BF16),
        cost_estimate=pl.CostEstimate(
            flops=flops, bytes_accessed=4 * fields.size, transcendentals=0
        ),
        name="forward",
    )(gain_own, shift_own, fields, mean, rstd, fwd_w, half_h)

    share = max(1, width // local_ch)
    pieces = [list(range(i, i + share)) for i in range(0, groups, share)]
    if share > 1:
        modes = lax.all_to_all(
            modes, "grid", split_axis=2, concat_axis=0, axis_index_groups=pieces, tiled=True
        )
    own_blocks = modes.shape[0] // width
    first_block = start // width
    own = lambda w, axis: lax.dynamic_slice_in_dim(w, first_block, own_blocks, axis)
    rep = max(1, 256 // (2 * width))
    w1 = real_form(own(first_weight, 1), rep)
    w2 = real_form(own(second_weight, 1), rep)
    bias = jnp.swapaxes(own(first_bias.reshape(2, -1, width), 1), 0, 1).reshape(own_blocks, -1)
    bias = jnp.tile(bias, (1, rep))[:, :, None]
    has_zero = (position % share == 0).astype(jnp.int32).reshape(1)
    own_k = modes.shape[2]
    kt = min(16, own_k)
    size = rep * 2 * width
    tile = pl.BlockSpec((width, 2, kt, cols), lambda b, k: (b, 0, k, 0))
    per_block = lambda n: pl.BlockSpec((1, size, n), lambda b, k: (b, 0, 0))
    scratch = pltpu.VMEM((2, cols // LANES, width * kt, LANES), F32)
    mixed = pl.pallas_call(
        functools.partial(mix_kernel, rep=rep),
        grid=(own_blocks, own_k // kt),
        in_specs=[smem, tile, per_block(size), per_block(size), per_block(1)],
        out_specs=tile,
        out_shape=jax.ShapeDtypeStruct(modes.shape, BF16),
        scratch_shapes=[scratch, scratch],
        cost_estimate=pl.CostEstimate(
            flops=16 * width * modes.size, bytes_accessed=4 * modes.size, transcendentals=0
        ),
        name="mix",
    )(has_zero, modes, w1, w2, bias)
    if share > 1:
        mixed = lax.all_to_all(
            mixed, "grid", split_axis=0, concat_axis=2, axis_index_groups=pieces, tiled=True
        )
    return pl.pallas_call(
        inverse_kernel,
        grid=(local_ch,),
        in_specs=[one4, one, whole((rows, rows)), whole((cols, cols))],
        out_specs=one,
        out_shape=jax.ShapeDtypeStruct(fields.shape, BF16),
        cost_estimate=pl.CostEstimate(
            flops=flops, bytes_accessed=6 * fields.size, transcendentals=0
        ),
        name="inverse",
    )(mixed, fields, half_t, inv_w)


def solution(mesh):
    return jax.shard_map(
        per_device,
        mesh=mesh,
        in_specs=(P(("batch", "grid"), None, None), P(), P(), P(), P(), P()),
        out_specs=P(("batch", "grid"), None, None),
        check_vma=False,
    )
```
